512 devices in a mesh: sub: 8 (over y), row: 8 (over x, core), col: 8 (over z).
Axes of the slice: x: 4, y: 8, z: 8, core: 2. Of those that a mesh axis runs over, the one named last changes fastest.
Arguments:
- visibility: bfloat16 [2, 64, 512, 4096], P(None, 'sub', 'row', 'col'), may hold values from -13 to 13
- sky_model: bfloat16 [2, 64, 512, 4096], P(None, 'sub', 'row', 'col'), may hold values from -4 to 4, as said below
- antenna_flags: int32 [8, 512], P('sub'), may hold values 0 or 1
- gains_init: float32 [2, 64, 512], P(None, 'sub'), may hold values from -0.5 to 1.5
Outputs:
- gains: float32 [2, 64, 512], P(None, 'sub')
The draws below stay inside these ranges and needn't reach their ends.
Inputs may be any that keep to these rules, and one draw needn't show every extreme that they name: `sky_model`: model visibility parts lie between -4 and 4.
All inputs are finite; a program needn't handle non-finite values.
Results may differ from the reference program's by a relative error of at most 0.0003.
Values sent between devices are 32-bit elements.
A program may use at most 64 MiB of HBM per device.

```python
import jax
import jax.numpy as jnp
from jax import lax

ANTENNAS = 512
CH_SUB = 8
TIMES = 8
ITERS = 3
SUBBANDS = 8
CHANNELS = 64
N_SUB = 8


def sky_draw(key):
    full_shape = (CHANNELS, ANTENNAS, ANTENNAS, TIMES)
    model_re = jnp.clip(jax.random.normal(jax.random.fold_in(key, 11), full_shape, jnp.float32), -4.0, 4.0)
    model_im = jnp.clip(jax.random.normal(jax.random.fold_in(key, 21), full_shape, jnp.float32), -4.0, 4.0)
    base_re = jax.random.uniform(jax.random.fold_in(key, 12), (SUBBANDS, 1, ANTENNAS), jnp.float32, 0.6, 1.3)
    base_im = jax.random.uniform(jax.random.fold_in(key, 22), (SUBBANDS, 1, ANTENNAS), jnp.float32, -0.3, 0.3)
    wiggle = jax.random.uniform(jax.random.fold_in(key, 13), (SUBBANDS, CH_SUB, ANTENNAS), jnp.float32, -0.1, 0.1)
    gain_re = (base_re + wiggle).reshape(CHANNELS, ANTENNAS)
    gain_im = jnp.broadcast_to(base_im, (SUBBANDS, CH_SUB, ANTENNAS)).reshape(CHANNELS, ANTENNAS)
    pair_re = gain_re[:, :, None, None] * gain_re[:, None, :, None] + gain_im[:, :, None, None] * gain_im[:, None, :, None]
    pair_im = gain_im[:, :, None, None] * gain_re[:, None, :, None] - gain_re[:, :, None, None] * gain_im[:, None, :, None]
    noise_re = 0.2 * jnp.clip(jax.random.normal(jax.random.fold_in(key, 14), full_shape, jnp.float32), -4.0, 4.0)
    noise_im = 0.2 * jnp.clip(jax.random.normal(jax.random.fold_in(key, 24), full_shape, jnp.float32), -4.0, 4.0)
    observed_re = pair_re * model_re - pair_im * model_im + noise_re
    observed_im = pair_re * model_im + pair_im * model_re + noise_im
    flat_shape = (CHANNELS, ANTENNAS, ANTENNAS * TIMES)
    model_both = jnp.stack([model_re.reshape(flat_shape), model_im.reshape(flat_shape)], axis=0)
    observed_both = jnp.stack([observed_re.reshape(flat_shape), observed_im.reshape(flat_shape)], axis=0)
    return (model_both, observed_both)


def draw_visibility(key, part):
    return sky_draw(key)[1].astype(jnp.bfloat16)


def draw_sky_model(key, part):
    return sky_draw(key)[0].astype(jnp.bfloat16)


def plant(entries, key, low, high):
    index_at = [jax.random.randint(jax.random.fold_in(key, axis), (), 0, length) for axis, length in enumerate(entries.shape)]
    main_axis = entries.shape.index(max(entries.shape))
    neighbour = index_at[:main_axis] + [(index_at[main_axis] + 1) % entries.shape[main_axis]] + index_at[main_axis + 1:]
    return entries.at[tuple(index_at)].set(low).at[tuple(neighbour)].set(high)


def block_scale(own_key, extent, shards, smallest, top_value):
    level, own = 1.0, jax.random.fold_in(own_key, 6)
    for dim, shards_of in shards:
        draws = jnp.exp(jax.random.uniform(jax.random.fold_in(own, dim), (shards_of,), jnp.float32, smallest / len(shards), top_value / len(shards)))
        level = level * jnp.repeat(draws, extent[dim] // shards_of).reshape([-1 if axis == dim else 1 for axis in range(len(extent))])
    return level


def setup_inputs(seed: int = 0) -> dict:
    splits = jax.random.split(jax.random.key(seed), 5)
    return {
        "visibility": draw_visibility(jax.random.fold_in(splits[4], 71), 0),
        "sky_model": draw_sky_model(jax.random.fold_in(splits[4], 71), 0),
        "antenna_flags": plant((jax.random.randint(splits[2], (SUBBANDS, ANTENNAS), 0, 8) < 7).astype(jnp.int32), jax.random.fold_in(splits[2], 1), 0, 1),
        "gains_init": jnp.clip(-0.5 + 2.0 * jax.random.uniform(splits[3], (2, CHANNELS, ANTENNAS), jnp.float32) ** block_scale(splits[3], (2, CHANNELS, ANTENNAS), ((1, 8),), -0.2, 0.2), -0.5, 1.5),
    }


def reference(visibility, sky_model, antenna_flags, gains_init):
    flag_values = antenna_flags.astype(jnp.float32)
    chan_flags = jnp.repeat(flag_values, CH_SUB, axis=0)
    off_diagonal = jnp.float32(1.0) - jnp.eye(ANTENNAS, dtype=jnp.float32)

    def prepare(bundle):
        vis_real, vis_imag, model_real, model_imag, flag_slice = bundle
        shape_three = (ANTENNAS, ANTENNAS, TIMES)
        vis_re = vis_real.astype(jnp.float32).reshape(shape_three)
        vis_im = vis_imag.astype(jnp.float32).reshape(shape_three)
        mod_re = model_real.astype(jnp.float32).reshape(shape_three)
        mod_im = model_imag.astype(jnp.float32).reshape(shape_three)
        weight = flag_slice[:, None] * flag_slice[None, :] * off_diagonal
        cross_re = jnp.sum(vis_re * mod_re + vis_im * mod_im, axis=2) * weight
        cross_im = jnp.sum(vis_im * mod_re - vis_re * mod_im, axis=2) * weight
        power_sum = jnp.sum(mod_re * mod_re + mod_im * mod_im, axis=2) * weight
        return cross_re, cross_im, power_sum

    cross_re, cross_im, power_sum = lax.map(prepare, (visibility[0], visibility[1], sky_model[0], sky_model[1], chan_flags))

    def contract(matrix, vector):
        return jnp.einsum("cpq,cq->cp", matrix, vector, precision=lax.Precision.HIGHEST)

    gain_values = gains_init
    for step_index in range(ITERS):
        gain_re = gain_values[0]
        gain_im = gain_values[1]
        num_re = contract(cross_re, gain_re) - contract(cross_im, gain_im)
        num_im = contract(cross_re, gain_im) + contract(cross_im, gain_re)
        denominator = contract(power_sum, gain_re * gain_re + gain_im * gain_im) + 1.0
        quotient = jnp.stack([num_re / denominator, num_im / denominator], axis=0)
        updated = 0.5 * (quotient + gain_values)
        grouped = updated.reshape(2, N_SUB, CH_SUB, ANTENNAS)
        chan_mean = jnp.mean(grouped, axis=2)
        overall = jnp.mean(chan_mean, axis=1)
        gain_values = (grouped + 0.5 * (overall[:, None, None, :] - chan_mean[:, :, None, :])).reshape(2, CHANNELS, ANTENNAS)
    return gain_values
```

```python
import functools

import jax
import jax.numpy as jnp
from jax import lax
from jax.experimental import pallas as pl
from jax.experimental.pallas import tpu as pltpu
from jax.sharding import PartitionSpec as P

TIMES = 8
ITERS = 3
MESH = pl.DeviceIdType.MESH


def far_first(n):
    return sorted(range(1, n), key=lambda d: (-min(d, n - d), d))


def kernel(
    sizes,
    vis_ref, sky_ref, flag_ref, init_ref, out_ref,
    vis, sky, prod, cross_re, cross_im, power, spread,
    zsend, zbuf, ysend, ybuf, gsend, gbuf, pbuf, fsend, fbuf,
    in_sem, z_ssem, z_rsem, y_ssem, y_rsem, g_ssem, g_rsem, p_ssem, p_rsem, f_ssem, f_rsem,
):
    n_sub, n_row, n_col, block, channels = sizes
    half = channels // 2
    f32, bf16 = jnp.float32, jnp.bfloat16
    sub, row, col = lax.axis_index("sub"), lax.axis_index("row"), lax.axis_index("col")
    hub = row == col
    wide = block * TIMES
    lanes = 2 * block

    loads = []
    for c in [j + half * h for j in range(half) for h in range(2)]:
        for a, (src, dst) in enumerate(((vis_ref, vis), (sky_ref, sky))):
            copy = pltpu.make_async_copy(src.at[:, c], dst.at[:, c], in_sem.at[a, c])
            copy.start()
            loads.append(((a, c), copy))
    loads = dict(loads)

    barrier = pltpu.get_barrier_semaphore()
    for axis, me, n in (("col", col, n_col), ("sub", sub, n_sub), ("row", row, n_row)):
        for d in far_first(n):
            pl.semaphore_signal(barrier, inc=1, device_id={axis: lax.rem(me + d, n)}, device_id_type=MESH)

    lane = lax.broadcasted_iota(jnp.int32, (1, lanes), 1)
    low = lane < block

    def pick(array, index, n):
        total = jnp.where(index == 0, array[..., 0:block], 0.0)
        for k in range(1, n):
            total = total + jnp.where(index == k, array[..., k * block : (k + 1) * block], 0.0)
        return total

    init = pick(init_ref[...], col, n_col)
    start_gains = jnp.concatenate(
        [jnp.concatenate([init[i, :half], init[i, half:]], axis=1) for i in range(2)], axis=0
    )

    flags = flag_ref[...].astype(f32)
    row_flag = pick(flags, row, n_row)
    row_flag = jnp.concatenate([row_flag, row_flag], axis=1)
    col_flag = pick(flags, col, n_col)
    diagonal = lax.broadcasted_iota(jnp.int32, (block, block), 0) == lax.broadcasted_iota(
        jnp.int32, (block, block), 1
    )
    col_flag = jnp.sum(jnp.where(diagonal, col_flag, 0.0), axis=1, keepdims=True)
    q_id = col * block + lax.broadcasted_iota(jnp.int32, (block, lanes), 0)
    p_id = row * block + lax.rem(lax.broadcasted_iota(jnp.int32, (block, lanes), 1), block)
    weight = jnp.where(q_id != p_id, col_flag * row_flag, 0.0)

    rows_k = 6 * channels
    k_id = lax.broadcasted_iota(jnp.int32, (rows_k, channels * lanes), 0)
    n_id = lax.broadcasted_iota(jnp.int32, (rows_k, channels * lanes), 1)
    spread[...] = jnp.where(
        (lax.rem(k_id, channels) == n_id // lanes)
        & (lax.rem(k_id // channels, 2) == lax.rem(n_id, lanes) // block),
        1.0,
        0.0,
    ).astype(bf16)

    def expand(gains):
        both = jnp.concatenate([gains[:, :block], gains[:, block:]], axis=0)
        high = both.astype(bf16)
        rest = both - high.astype(f32)
        mid = rest.astype(bf16)
        last = (rest - mid.astype(f32)).astype(bf16)
        pieces = jnp.concatenate([high, mid, last], axis=0)
        return lax.dot_general(
            pieces, spread[...], (((0,), (0,)), ((), ())), preferred_element_type=f32
        )

    def contract(step, wide_gains, j):
        g_re = wide_gains[:, j * lanes : (j + 1) * lanes]
        g_im = wide_gains[:, (half + j) * lanes : (half + j + 1) * lanes]
        c_re, c_im, c_pow = cross_re[j], cross_im[j], power[j]
        zsend[step, j : j + 1] = jnp.sum(c_re * g_re - c_im * g_im, axis=0, keepdims=True)
        zsend[step, half + j : half + j + 1] = jnp.sum(c_re * g_im + c_im * g_re, axis=0, keepdims=True)
        zsend[step, channels + j : channels + j + 1] = jnp.sum(
            c_pow * (g_re * g_re + g_im * g_im), axis=0, keepdims=True
        )

    kt = 2
    deep = wide // kt
    out_rows = block // kt
    selector = jnp.where(
        lax.broadcasted_iota(jnp.int32, (out_rows, deep), 1) // TIMES
        == lax.broadcasted_iota(jnp.int32, (out_rows, deep), 0),
        1.0,
        0.0,
    ).astype(bf16)
    first_gains = expand(start_gains)
    for j in range(half):
        for h in range(2):
            c = j + half * h
            loads[(0, c)].wait()
            loads[(1, c)].wait()
            v_re, v_im = vis[0, c].astype(f32), vis[1, c].astype(f32)
            m_re, m_im = sky[0, c].astype(f32), sky[1, c].astype(f32)
            for i, value in enumerate(
                (v_re * m_re + v_im * m_im, v_im * m_re - v_re * m_im, m_re * m_re + m_im * m_im)
            ):
                high = value.astype(bf16)
                prod[i, h * block : (h + 1) * block] = high
                prod[i, lanes + h * block : lanes + (h + 1) * block] = (value - high.astype(f32)).astype(bf16)
        for i, dst in enumerate((cross_re, cross_im, power)):
            for t in range(kt):
                total = lax.dot_general(
                    selector,
                    prod[i, :, t * deep : (t + 1) * deep],
                    (((1,), (1,)), ((), ())),
                    preferred_element_type=f32,
                )
                rows = slice(t * out_rows, (t + 1) * out_rows)
                dst[j, rows] = (total[:, :lanes] + total[:, lanes:]) * weight[rows]
        contract(0, first_gains, j)

    pl.semaphore_wait(barrier, n_col + n_sub + n_row - 3)

    def copy_of(src, dst, ssem, rsem, axis, peer):
        return pltpu.make_async_remote_copy(
            src_ref=src, dst_ref=dst, send_sem=ssem, recv_sem=rsem,
            device_id={axis: peer}, device_id_type=MESH,
        )

    def update(total, previous):
        den = total[channels:] + 1.0
        quotient = total[:channels] / jnp.concatenate([den, den], axis=0)
        return 0.5 * (quotient + previous)

    def mean_of(updated):
        re = jnp.sum(updated[:half], axis=0, keepdims=True)
        im = jnp.sum(updated[half:], axis=0, keepdims=True)
        packed = jnp.where(low, re, im)
        other = jnp.where(low, im, re)
        return (packed + pltpu.roll(other, block, 1)) / channels

    def over_sub(step, updated):
        mean = mean_of(updated)
        ysend[step] = mean
        copies = []
        for d in far_first(n_sub):
            copy = copy_of(
                ysend.at[step], ybuf.at[step, sub], y_ssem.at[step, d], y_rsem.at[step, sub],
                "sub", lax.rem(sub + d, n_sub),
            )
            copy.start()
            copies.append(copy)
        total = mean
        for d in range(1, n_sub):
            peer = lax.rem(sub + d, n_sub)
            copy_of(ysend.at[step], ybuf.at[step, peer], y_ssem.at[step, d], y_rsem.at[step, peer],
                    "sub", peer).wait_recv()
            total = total + ybuf[step, peer]
        delta = 0.5 * (total / n_sub - mean)
        turned = pltpu.roll(delta, block, 1)
        d_re = jnp.where(low, delta, turned)
        d_im = jnp.where(low, turned, delta)
        shift = jnp.concatenate(
            [jnp.broadcast_to(d_re, (half, lanes)), jnp.broadcast_to(d_im, (half, lanes))], axis=0
        )
        for copy in copies:
            copy.wait_send()
        return updated + shift

    for step in range(ITERS - 1):
        def to_hub(step=step):
            return copy_of(zsend.at[step], zbuf.at[step, col], z_ssem.at[step, 0], z_rsem.at[step, col],
                           "col", row)

        @pl.when(jnp.logical_not(hub))
        def _(step=step):
            to_hub().start()

        @pl.when(hub)
        def _(step=step):
            total = zsend[step]
            for d in range(1, n_col):
                peer = lax.rem(col + d, n_col)
                copy_of(zsend.at[step], zbuf.at[step, peer], z_ssem.at[step, 0], z_rsem.at[step, peer],
                        "col", peer).wait_recv()
                total = total + zbuf[step, peer]
            previous = start_gains if step == 0 else gsend[step - 1]
            gains = over_sub(step, update(total, previous))
            gsend[step] = gains
            copies = []
            for d in far_first(n_row):
                copy = copy_of(gsend.at[step], gbuf.at[step], g_ssem.at[step, d], g_rsem.at[step],
                               "row", lax.rem(row + d, n_row))
                copy.start()
                copies.append(copy)
            if step == ITERS - 2:
                for d in far_first(n_col):
                    copy = copy_of(gsend.at[step], pbuf, p_ssem.at[d], p_rsem, "col", lax.rem(col + d, n_col))
                    copy.start()
                    copies.append(copy)
                pbuf[...] = gains
            gbuf[step] = gains
            for copy in copies:
                copy.wait_send()

        @pl.when(jnp.logical_not(hub))
        def _(step=step):
            copy_of(gsend.at[step], gbuf.at[step], g_ssem.at[step, 0], g_rsem.at[step], "row", col).wait_recv()
            to_hub().wait_send()

        wide_gains = expand(gbuf[step])
        for j in range(half):
            contract(step + 1, wide_gains, j)

    step = ITERS - 1
    copies = []
    for d in far_first(n_col):
        copy = copy_of(zsend.at[step], zbuf.at[step, col], z_ssem.at[step, d], z_rsem.at[step, col],
                       "col", lax.rem(col + d, n_col))
        copy.start()
        copies.append(copy)

    @pl.when(jnp.logical_not(hub))
    def _():
        copy_of(gsend.at[0], pbuf, p_ssem.at[0], p_rsem, "col", row).wait_recv()

    total = zsend[step]
    for d in range(1, n_col):
        peer = lax.rem(col + d, n_col)
        copy_of(zsend.at[step], zbuf.at[step, peer], z_ssem.at[step, d], z_rsem.at[step, peer],
                "col", peer).wait_recv()
        total = total + zbuf[step, peer]
    gains = over_sub(step, update(total, pbuf[...]))
    fsend[...] = gains
    for d in far_first(n_row):
        copy = copy_of(fsend, fbuf.at[row], f_ssem.at[d], f_rsem.at[row], "row", lax.rem(row + d, n_row))
        copy.start()
        copies.append(copy)
    fbuf[row] = gains
    for d in range(1, n_row):
        peer = lax.rem(row + d, n_row)
        copy_of(fsend, fbuf.at[peer], f_ssem.at[d], f_rsem.at[peer], "row", peer).wait_recv()
    for m in range(n_row // 2):
        a, b = fbuf[2 * m], fbuf[2 * m + 1]
        first = jnp.where(low, a, pltpu.roll(b, block, 1))
        second = jnp.where(low, pltpu.roll(a, block, 1), b)
        at = slice(m * lanes, (m + 1) * lanes)
        for i in range(2):
            out_ref[i, :, at] = jnp.concatenate(
                [first[i * half : (i + 1) * half], second[i * half : (i + 1) * half]], axis=0
            )
    for copy in copies:
        copy.wait_send()


def body(visibility, sky_model, antenna_flags, gains_init):
    n_sub, n_row, n_col = (lax.axis_size(axis) for axis in ("sub", "row", "col"))
    _, channels, block, wide = visibility.shape
    lanes = 2 * block
    half = channels // 2
    f32, bf16 = jnp.float32, jnp.bfloat16
    dma = pltpu.SemaphoreType.DMA
    return pl.pallas_call(
        functools.partial(kernel, (n_sub, n_row, n_col, block, channels)),
        out_shape=jax.ShapeDtypeStruct(gains_init.shape, f32),
        in_specs=[
            pl.BlockSpec(memory_space=pl.ANY),
            pl.BlockSpec(memory_space=pl.ANY),
            pl.BlockSpec(memory_space=pltpu.VMEM),
            pl.BlockSpec(memory_space=pltpu.VMEM),
        ],
        out_specs=pl.BlockSpec(memory_space=pltpu.VMEM),
        scratch_shapes=[
            pltpu.VMEM(visibility.shape, bf16),
            pltpu.VMEM(visibility.shape, bf16),
            pltpu.VMEM((3, 2 * lanes, wide), bf16),
            pltpu.VMEM((half, block, lanes), f32),
            pltpu.VMEM((half, block, lanes), f32),
            pltpu.VMEM((half, block, lanes), f32),
            pltpu.VMEM((6 * channels, channels * lanes), bf16),
            pltpu.VMEM((ITERS, 3 * half, lanes), f32),
            pltpu.VMEM((ITERS, n_col, 3 * half, lanes), f32),
            pltpu.VMEM((ITERS, 1, lanes), f32),
            pltpu.VMEM((ITERS, n_sub, 1, lanes), f32),
            pltpu.VMEM((ITERS - 1, channels, lanes), f32),
            pltpu.VMEM((ITERS - 1, channels, lanes), f32),
            pltpu.VMEM((channels, lanes), f32),
            pltpu.VMEM((channels, lanes), f32),
            pltpu.VMEM((n_row, channels, lanes), f32),
            dma((2, channels)),
            dma((ITERS, n_col)),
            dma((ITERS, n_col)),
            dma((ITERS, n_sub)),
            dma((ITERS, n_sub)),
            dma((ITERS - 1, n_row)),
            dma((ITERS - 1,)),
            dma((n_col,)),
            dma,
            dma((n_row,)),
            dma((n_row,)),
        ],
        compiler_params=pltpu.CompilerParams(collective_id=0, has_side_effects=True),
        name="stefcal",
    )(visibility, sky_model, antenna_flags, gains_init)


def solution(mesh):
    return jax.shard_map(
        body,
        mesh=mesh,
        in_specs=(
            P(None, "sub", "row", "col"),
            P(None, "sub", "row", "col"),
            P("sub", None),
            P(None, "sub", None),
        ),
        out_specs=P(None, "sub", None),
        check_vma=False,
    )
```
